256 devices in a mesh: row: 16 (over z_hi, x, core), col: 16 (over y, z_lo).
Axes of the slice: x: 4, y: 4, z: 8 (z_hi: 2, z_lo: 4; z = z_hi * 4 + z_lo), core: 2. Of those that a mesh axis runs over, the one named last changes fastest.
Arguments:
- covariance: float32 [16384, 16384], P('row', 'col'), may hold values from -10 to 14, as said below
- wind_x: float32 [128, 128], replicated, may hold values from -0.2 to 0.2
- wind_y: float32 [128, 128], replicated, may hold values from -0.2 to 0.2
- patch_map: int32 [128, 128], replicated, may hold values from 0 to 15
- kappa_table: float32 [16], replicated, may hold values from 0.1 to 0.24
Outputs:
- forecast: float32 [16384, 16384], P('row', 'col')
The draws below stay inside these ranges and needn't reach their ends.
Inputs may be any that keep to these rules, and one draw needn't show every extreme that they name: covariance is symmetric.
All inputs are finite; a program needn't handle non-finite values.
Results may differ from the reference program's by a relative error of at most 0.00002.
Values sent between devices are 32-bit elements; how exact they have to be, the bound alone decides.
A program may use at most 64 MiB of HBM per device.

```python
import math
import jax
import jax.numpy as jnp

GY = 128
SUBSTEPS = 4
PATCHES = 16
GX = 128
ORDER = 16384


def draw_covariance(key, part):
    noise = jax.random.normal(jax.random.fold_in(key, 11), (ORDER, ORDER), jnp.float32)
    symmetric = 0.5 * (noise + noise.T)
    return symmetric + 2.0 * jnp.eye(ORDER, dtype=jnp.float32)


def plant(array, rng, least, largest):
    extent = array.shape
    place = [jax.random.randint(jax.random.fold_in(rng, axis), (), 0, extent[axis]) for axis in range(len(extent))]
    array = array.at[tuple(place)].set(least)
    longest = extent.index(max(extent))
    place[longest] = (place[longest] + 1) % extent[longest]
    return array.at[tuple(place)].set(largest)


def setup_inputs(seed: int = 0) -> dict:
    key_list = jax.random.split(jax.random.key(seed), 6)
    covariance = draw_covariance(jax.random.fold_in(key_list[5], 71), 0)
    wind_x = jnp.clip(jax.random.uniform(key_list[1], (GX, GY), jnp.float32, -0.2, 0.2), -0.2, 0.2)
    wind_y = jnp.clip(jax.random.uniform(key_list[2], (GX, GY), jnp.float32, -0.2, 0.2), -0.2, 0.2)
    patch_map = plant(jax.random.randint(key_list[3], (GX, GY), 0, PATCHES), jax.random.fold_in(key_list[3], 1), 0, PATCHES - 1).astype(jnp.int32)
    kappa_table = jnp.clip(jnp.exp(jax.random.uniform(key_list[4], (PATCHES,), jnp.float32, math.log(0.1), math.log(0.24))), 0.1, 0.24)
    return dict(covariance=covariance, wind_x=wind_x, wind_y=wind_y, patch_map=patch_map, kappa_table=kappa_table)


def coefficient_maps(wind_x, wind_y, patch_map, kappa_table):
    labels = jnp.arange(PATCHES, dtype=jnp.int32)
    member = (patch_map[:, :, None] == labels).astype(jnp.float32)
    diffusivity = jnp.sum(member * kappa_table, axis=-1)
    return (1.0 - 4.0 * diffusivity, diffusivity - 0.5 * wind_x, diffusivity + 0.5 * wind_x,
            diffusivity - 0.5 * wind_y, diffusivity + 0.5 * wind_y)


def advance_rows(current, weights):
    padded = jnp.pad(current, ((1, 1), (1, 1), (0, 0)))
    centre, north, south, east, west = [weight[:, :, None] for weight in weights]
    return (centre * current + north * padded[2:, 1:-1] + south * padded[:-2, 1:-1]
            + east * padded[1:-1, 2:] + west * padded[1:-1, :-2])


def advance_columns(current, weights):
    padded = jnp.pad(current, ((0, 0), (1, 1), (1, 1)))
    centre, north, south, east, west = weights
    return (centre * current + north * padded[:, 2:, 1:-1] + south * padded[:, :-2, 1:-1]
            + east * padded[:, 1:-1, 2:] + west * padded[:, 1:-1, :-2])


def reference(covariance, wind_x, wind_y, patch_map, kappa_table):
    grid_rows = wind_x.shape[0]
    cells_total = grid_rows * GY
    weights = coefficient_maps(wind_x, wind_y, patch_map, kappa_table)
    current = covariance.reshape(grid_rows, GY, cells_total)
    for _ in range(SUBSTEPS):
        current = advance_rows(current, weights)
    current = current.reshape(cells_total, grid_rows, GY)
    for _ in range(SUBSTEPS):
        current = advance_columns(current, weights)
    return current.reshape(cells_total, cells_total)
```

```python
import jax
import jax.numpy as jnp
from jax import lax
from jax.experimental import pallas as pl
from jax.experimental.pallas import tpu as pltpu
from jax.sharding import PartitionSpec as P

GY = 128
PATCHES = 16
MESH = pl.DeviceIdType.MESH
ORDER = (0, 7, 1, 6, 2, 5, 3, 4)
HALF = 512


def coefficients(wind_x, wind_y, patch_map, kappa_table):
    kappa = jnp.zeros((GY, GY), jnp.float32)
    for label in range(PATCHES):
        kappa = jnp.where(patch_map[...] == label, kappa_table[label], kappa)
    y = lax.broadcasted_iota(jnp.int32, (GY, GY), 1)
    half_x, half_y = 0.5 * wind_x[...], 0.5 * wind_y[...]
    return (
        1.0 - 4.0 * kappa,
        kappa - half_x,
        kappa + half_x,
        jnp.where(y < GY - 1, kappa - half_y, 0.0),
        jnp.where(y > 0, kappa + half_y, 0.0),
    )


def kernel(
    cov, wind_x, wind_y, patch_map, kappa_table, out,
    wide, f0, f1, f2, f3, final, lane_coef, sub_coef, padded,
    own_sem, out_sem, col_send, col_recv, row_send, row_recv,
):
    r, c = lax.axis_index("row"), lax.axis_index("col")
    rows, cols = lax.axis_size("row"), lax.axis_size("col")
    has = {"up": r > 0, "down": r < rows - 1, "left": c > 0, "right": c < cols - 1}
    where = {"up": (r - 1, c), "down": (r + 1, c), "left": (r, c - 1), "right": (r, c + 1)}

    own = [
        pltpu.make_async_copy(
            cov.at[pl.ds(k * GY, GY), :], wide.at[pl.ds(k * GY, GY), pl.ds(HALF, 1024)], own_sem.at[k]
        )
        for k in range(8)
    ]
    for k in ORDER:
        own[k].start()

    barrier = pltpu.get_barrier_semaphore()
    for side in has:
        @pl.when(has[side])
        def _():
            pl.semaphore_signal(barrier, inc=1, device_id=where[side], device_id_type=MESH)
    pl.semaphore_wait(barrier, sum(there.astype(jnp.int32) for there in has.values()))

    def col_copy(side, k):
        i = 0 if side == "left" else 1
        return pltpu.make_async_remote_copy(
            src_ref=cov.at[pl.ds(k * GY, GY), pl.ds(HALF * i, HALF)],
            dst_ref=wide.at[pl.ds(k * GY, GY), pl.ds(1536 if i == 0 else 0, HALF)],
            send_sem=col_send.at[i, k],
            recv_sem=col_recv.at[i, k],
            device_id=where[side],
            device_id_type=MESH,
        )

    def row_copy(k):
        side = "up" if k < 4 else "down"
        return pltpu.make_async_remote_copy(
            src_ref=f0.at[4 + k],
            dst_ref=f0.at[12 + k if k < 4 else k - 4],
            send_sem=row_send.at[k],
            recv_sem=row_recv.at[k],
            device_id=where[side],
            device_id_type=MESH,
        )

    for k in ORDER:
        for side in ("left", "right"):
            @pl.when(has[side])
            def _():
                col_copy(side, k).start()

    maps = coefficients(wind_x, wind_y, patch_map, kappa_table)
    padded[...] = jnp.zeros_like(padded)
    for j in range(5):
        padded[j, pl.ds(8, GY), :] = maps[j]
    for j in range(5):
        window = padded[j, pl.ds(pl.multiple_of(8 * c, 8), 24), :]
        for w in range(14):
            lane_coef[j, w] = jnp.broadcast_to(window[5 + w : 6 + w, :], (8, GY))
    for j in range(5):
        turned = pltpu.roll(maps[j].T, lax.rem(132 - 8 * r, 128), 1)
        for w in range(14):
            place = 8 * r - 3 + w
            inside = jnp.logical_and(place >= 0, place < GY)
            column = jnp.broadcast_to(turned[:, w + 1 : w + 2], (GY, GY))
            sub_coef[w, j] = jnp.where(inside, column, 0.0)

    @pl.when(c == 0)
    def _():
        wide[:, pl.ds(0, HALF)] = jnp.zeros((1024, HALF), jnp.float32)

    @pl.when(c == cols - 1)
    def _():
        wide[:, pl.ds(1536, HALF)] = jnp.zeros((1024, HALF), jnp.float32)

    @pl.when(r == 0)
    def _():
        f0[pl.ds(0, 4)] = jnp.zeros((4, GY, 1024), jnp.float32)

    @pl.when(r == rows - 1)
    def _():
        f0[pl.ds(12, 4)] = jnp.zeros((4, GY, 1024), jnp.float32)

    def col_phase(k):
        def group(i, carry):
            base = pl.multiple_of(k * GY + i * 16, 16)
            inner = pl.multiple_of(i * 16, 16)
            slabs = [
                [wide[pl.ds(base + 8 * u, 8), pl.ds(GY * w, GY)] for u in range(2)] for w in range(16)
            ]
            for s in range(4):
                fresh = [None] * 16
                for w in range(s + 1, 15 - s):
                    cc, cn, cs, ce, cw = [lane_coef[j, w - 1] for j in range(5)]
                    fresh[w] = [
                        cc * slabs[w][u]
                        + cn * slabs[w + 1][u]
                        + cs * slabs[w - 1][u]
                        + ce * pltpu.roll(slabs[w][u], GY - 1, 1)
                        + cw * pltpu.roll(slabs[w][u], 1, 1)
                        for u in range(2)
                    ]
                slabs = fresh
            for w in range(4, 12):
                for u in range(2):
                    f0[4 + k, pl.ds(inner + 8 * u, 8), pl.ds(GY * (w - 4), GY)] = slabs[w][u]
            return carry

        lax.fori_loop(0, 8, group, 0)

    sub = lax.broadcasted_iota(jnp.int32, (8, GY), 0)

    def row_task(source, target, shift, g):
        def part(q, carry):
            lanes = [pl.ds(pl.multiple_of(q * 256 + GY * u, GY), GY) for u in range(2)]

            def load(grid, k, u):
                return source[grid, pl.ds(8 * k, 8), lanes[u]]

            here = [[load(g, 0, u) for u in range(2)]]
            ups = [[pltpu.roll(here[0][u], 7, 0) for u in range(2)]]
            last_down = [jnp.zeros((8, GY), jnp.float32)] * 2
            for k in range(16):
                if k < 15:
                    here.append([load(g, k + 1, u) for u in range(2)])
                    ups.append([pltpu.roll(here[k + 1][u], 7, 0) for u in range(2)])
                cc, cn, cs, ce, cw = [sub_coef[g - 1, j, pl.ds(8 * k, 8), :] for j in range(5)]
                for u in range(2):
                    down = pltpu.roll(here[k][u], 1, 0)
                    east = jnp.where(sub == 7, ups[k + 1][u], ups[k][u]) if k < 15 else ups[k][u]
                    west = jnp.where(sub == 0, last_down[u], down)
                    last_down[u] = down
                    target[g - shift, pl.ds(8 * k, 8), lanes[u]] = (
                        cc * here[k][u]
                        + cn * load(g + 1, k, u)
                        + cs * load(g - 1, k, u)
                        + ce * east
                        + cw * west
                    )
            return carry

        lax.fori_loop(0, 4, part, 0)

    for k in ORDER:
        own[k].wait()
        for side in ("left", "right"):
            source_side = "right" if side == "left" else "left"

            @pl.when(has[source_side])
            def _():
                col_copy(side, k).wait_recv()

        col_phase(k)

        @pl.when(has["up" if k < 4 else "down"])
        def _():
            row_copy(k).start()

    for k in ORDER:
        @pl.when(has["down" if k < 4 else "up"])
        def _():
            row_copy(k).wait_recv()

    fields = (f0, f1, f2, f3)
    for s in range(3):
        lax.fori_loop(s + 1, 15 - s, lambda g, x, s=s: row_task(fields[s], fields[s + 1], 0, g) or x, 0)

    def finish(g, carry):
        row_task(f3, final, 4, g)
        pltpu.make_async_copy(
            final.at[g - 4], out.at[pl.ds(pl.multiple_of((g - 4) * GY, GY), GY), :], out_sem.at[g - 4]
        ).start()
        return carry

    lax.fori_loop(4, 12, finish, 0)
    for k in range(8):
        pltpu.make_async_copy(final.at[k], out.at[pl.ds(k * GY, GY), :], out_sem.at[k]).wait()
        for side in ("left", "right"):
            @pl.when(has[side])
            def _():
                col_copy(side, k).wait_send()

        @pl.when(has["up" if k < 4 else "down"])
        def _():
            row_copy(k).wait_send()


def per_device(covariance, wind_x, wind_y, patch_map, kappa_table):
    f32 = jnp.float32
    dma = pltpu.SemaphoreType.DMA
    return pl.pallas_call(
        kernel,
        out_shape=jax.ShapeDtypeStruct(covariance.shape, f32),
        in_specs=[
            pl.BlockSpec(memory_space=pl.ANY),
            pl.BlockSpec(memory_space=pltpu.VMEM),
            pl.BlockSpec(memory_space=pltpu.VMEM),
            pl.BlockSpec(memory_space=pltpu.VMEM),
            pl.BlockSpec(memory_space=pltpu.SMEM),
        ],
        out_specs=pl.BlockSpec(memory_space=pl.ANY),
        scratch_shapes=[
            pltpu.VMEM((1024, 2048), f32),
            pltpu.VMEM((16, GY, 1024), f32),
            pltpu.VMEM((16, GY, 1024), f32),
            pltpu.VMEM((16, GY, 1024), f32),
            pltpu.VMEM((16, GY, 1024), f32),
            pltpu.VMEM((8, GY, 1024), f32),
            pltpu.VMEM((5, 14, 8, GY), f32),
            pltpu.VMEM((14, 5, GY, GY), f32),
            pltpu.VMEM((5, 144, GY), f32),
            dma((8,)),
            dma((8,)),
            dma((2, 8)),
            dma((2, 8)),
            dma((8,)),
            dma((8,)),
        ],
        compiler_params=pltpu.CompilerParams(
            collective_id=0, has_side_effects=True, vmem_limit_bytes=62 * 1024 * 1024
        ),
    )(covariance, wind_x, wind_y, patch_map, kappa_table)


def solution(mesh):
    return jax.shard_map(
        per_device,
        mesh=mesh,
        in_specs=(P("row", "col"), P(), P(), P(), P()),
        out_specs=P("row", "col"),
        check_vma=False,
    )
```

```python
import jax
import jax.numpy as jnp
from jax import lax
from jax.experimental import pallas as pl
from jax.experimental.pallas import tpu as pltpu
from jax.sharding import PartitionSpec as P

GY = 128
PATCHES = 16
MESH = pl.DeviceIdType.MESH
AHEAD = 2
HALF = 512


def coefficients(wind_x, wind_y, patch_map, kappa_table):
    kappa = jnp.zeros((GY, GY), jnp.float32)
    for label in range(PATCHES):
        kappa = jnp.where(patch_map[...] == label, kappa_table[label], kappa)
    y = lax.broadcasted_iota(jnp.int32, (GY, GY), 1)
    half_x, half_y = 0.5 * wind_x[...], 0.5 * wind_y[...]
    return (
        1.0 - 4.0 * kappa,
        kappa - half_x,
        kappa + half_x,
        jnp.where(y < GY - 1, kappa - half_y, 0.0),
        jnp.where(y > 0, kappa + half_y, 0.0),
    )


def kernel(
    cov, wind_x, wind_y, patch_map, kappa_table, out,
    wide, f0, f1, f2, f3, final, relay, lane_coef, sub_coef, padded,
    own_sem, out_sem, col_send, col_recv, far_send, far_recv, near_send, near_recv,
    relay_send, relay_recv,
):
    r, c = lax.axis_index("row"), lax.axis_index("col")
    rows, cols = lax.axis_size("row"), lax.axis_size("col")
    odd = lax.rem(r, 2)

    def pick(even_value, odd_value):
        return even_value + odd * (odd_value - even_value)

    near_row, far_row = pick(r + 1, r - 1), pick(r - 1, r + 1)
    has_far = jnp.logical_and(r > 0, r < rows - 1)
    middle = jnp.logical_or(r == 7, r == 8)
    direct = jnp.logical_and(has_far, jnp.logical_not(middle))
    relay_col = 12 * lax.rem(c, 2) + lax.rem(c, 4)
    sent_to = (9 * (r - 7) + 2 * (c // 4), relay_col)
    taken_from = (9 * (8 - r) + 2 * (c // 4), relay_col)
    is_relay = jnp.logical_and(c == relay_col, r // 8 == odd)
    flow_col = 4 * (lax.rem(r, 8) // 2) + lax.rem(c, 4)
    flow_from, flow_to = (7 + r // 8, flow_col), (8 - r // 8, flow_col)
    has = {"left": c > 0, "right": c < cols - 1}
    where = {"left": (r, c - 1), "right": (r, c + 1)}

    def chunk(step):
        return pick(step, 7 - step)

    def chunk_rows(step):
        return pl.ds(pl.multiple_of(chunk(step) * GY, GY), GY)

    def own_copy(step):
        return pltpu.make_async_copy(
            cov.at[chunk_rows(step), :], wide.at[chunk_rows(step), pl.ds(HALF, 1024)], own_sem.at[step]
        )

    for step in range(8):
        own_copy(step).start()

    barrier = pltpu.get_barrier_semaphore()
    peers = (
        (has["left"], where["left"]),
        (has["right"], where["right"]),
        (r >= 0, (near_row, c)),
        (direct, (far_row, c)),
        (middle, sent_to),
        (middle, taken_from),
        (is_relay, flow_from),
        (is_relay, flow_to),
    )
    for there, peer in peers:
        @pl.when(there)
        def _():
            pl.semaphore_signal(barrier, inc=1, device_id=peer, device_id_type=MESH)
    pl.semaphore_wait(barrier, sum(there.astype(jnp.int32) for there, _ in peers))

    def col_copy(side, step):
        i = 0 if side == "left" else 1
        return pltpu.make_async_remote_copy(
            src_ref=cov.at[chunk_rows(step), pl.ds(HALF * i, HALF)],
            dst_ref=wide.at[chunk_rows(step), pl.ds(1536 if i == 0 else 0, HALF)],
            send_sem=col_send.at[i, step],
            recv_sem=col_recv.at[i, step],
            device_id=where[side],
            device_id_type=MESH,
        )

    def send_columns(step):
        for side in ("left", "right"):
            @pl.when(has[side])
            def _():
                col_copy(side, step).start()

    def far_copy(step):
        return pltpu.make_async_remote_copy(
            src_ref=f0.at[4 + chunk(step)],
            dst_ref=f0.at[pick(12 + step, 3 - step)],
            send_sem=far_send.at[step],
            recv_sem=far_recv.at[step],
            device_id=(far_row, c),
            device_id_type=MESH,
        )

    def to_relay(step):
        return pltpu.make_async_remote_copy(
            src_ref=f0.at[4 + chunk(step)],
            dst_ref=relay.at[step],
            send_sem=far_send.at[step],
            recv_sem=relay_recv.at[step],
            device_id=sent_to,
            device_id_type=MESH,
        )

    def from_relay(step):
        return pltpu.make_async_remote_copy(
            src_ref=relay.at[step],
            dst_ref=f0.at[pick(3 - step, 12 + step)],
            send_sem=relay_send.at[step],
            recv_sem=far_recv.at[step],
            device_id=flow_to,
            device_id_type=MESH,
        )

    def near_copy(step):
        return pltpu.make_async_remote_copy(
            src_ref=f0.at[4 + chunk(step)],
            dst_ref=f0.at[pick(step - 4, 19 - step)],
            send_sem=near_send.at[step - 4],
            recv_sem=near_recv.at[step - 4],
            device_id=(near_row, c),
            device_id_type=MESH,
        )

    for step in range(AHEAD):
        send_columns(step)

    maps = coefficients(wind_x, wind_y, patch_map, kappa_table)
    padded[...] = jnp.zeros_like(padded)
    for j in range(5):
        padded[j, pl.ds(8, GY), :] = maps[j]
    for j in range(5):
        window = padded[j, pl.ds(pl.multiple_of(8 * c, 8), 24), :]
        for w in range(14):
            lane_coef[j, w] = jnp.broadcast_to(window[5 + w : 6 + w, :], (8, GY))
    for j in range(5):
        turned = pltpu.roll(maps[j].T, lax.rem(132 - 8 * r, 128), 1)
        for w in range(14):
            place = 8 * r - 3 + w
            inside = jnp.logical_and(place >= 0, place < GY)
            column = jnp.broadcast_to(turned[:, w + 1 : w + 2], (GY, GY))
            sub_coef[w, j] = jnp.where(inside, column, 0.0)

    @pl.when(c == 0)
    def _():
        wide[:, pl.ds(0, HALF)] = jnp.zeros((1024, HALF), jnp.float32)

    @pl.when(c == cols - 1)
    def _():
        wide[:, pl.ds(1536, HALF)] = jnp.zeros((1024, HALF), jnp.float32)

    @pl.when(r == 0)
    def _():
        f0[pl.ds(0, 4)] = jnp.zeros((4, GY, 1024), jnp.float32)

    @pl.when(r == rows - 1)
    def _():
        f0[pl.ds(12, 4)] = jnp.zeros((4, GY, 1024), jnp.float32)

    def col_phase(step):
        k = chunk(step)

        def group(i, carry):
            base = pl.multiple_of(k * GY + i * 16, 16)
            inner = pl.multiple_of(i * 16, 16)
            slabs = [
                [wide[pl.ds(base + 8 * u, 8), pl.ds(GY * w, GY)] for u in range(2)] for w in range(16)
            ]
            for s in range(4):
                fresh = [None] * 16
                for w in range(s + 1, 15 - s):
                    cc, cn, cs, ce, cw = [lane_coef[j, w - 1] for j in range(5)]
                    fresh[w] = [
                        cc * slabs[w][u]
                        + cn * slabs[w + 1][u]
                        + cs * slabs[w - 1][u]
                        + ce * pltpu.roll(slabs[w][u], GY - 1, 1)
                        + cw * pltpu.roll(slabs[w][u], 1, 1)
                        for u in range(2)
                    ]
                slabs = fresh
            for w in range(4, 12):
                for u in range(2):
                    f0[4 + k, pl.ds(inner + 8 * u, 8), pl.ds(GY * (w - 4), GY)] = slabs[w][u]
            return carry

        lax.fori_loop(0, 8, group, 0)

    sub = lax.broadcasted_iota(jnp.int32, (8, GY), 0)

    def row_task(source, target, shift, g):
        def part(q, carry):
            lanes = [pl.ds(pl.multiple_of(q * 256 + GY * u, GY), GY) for u in range(2)]

            def load(grid, k, u):
                return source[grid, pl.ds(8 * k, 8), lanes[u]]

            here = [[load(g, 0, u) for u in range(2)]]
            ups = [[pltpu.roll(here[0][u], 7, 0) for u in range(2)]]
            last_down = [jnp.zeros((8, GY), jnp.float32)] * 2
            for k in range(16):
                if k < 15:
                    here.append([load(g, k + 1, u) for u in range(2)])
                    ups.append([pltpu.roll(here[k + 1][u], 7, 0) for u in range(2)])
                cc, cn, cs, ce, cw = [sub_coef[g - 1, j, pl.ds(8 * k, 8), :] for j in range(5)]
                for u in range(2):
                    down = pltpu.roll(here[k][u], 1, 0)
                    east = jnp.where(sub == 7, ups[k + 1][u], ups[k][u]) if k < 15 else ups[k][u]
                    west = jnp.where(sub == 0, last_down[u], down)
                    last_down[u] = down
                    target[g - shift, pl.ds(8 * k, 8), lanes[u]] = (
                        cc * here[k][u]
                        + cn * load(g + 1, k, u)
                        + cs * load(g - 1, k, u)
                        + ce * east
                        + cw * west
                    )
            return carry

        lax.fori_loop(0, 4, part, 0)

    def out_copy(g):
        return pltpu.make_async_copy(
            final.at[g - 4], out.at[pl.ds(pl.multiple_of((g - 4) * GY, GY), GY), :], out_sem.at[g - 4]
        )

    fields = (f0, f1, f2, f3, final)

    def row_phase(first, last, slope):
        for s in range(4):
            def task(i, carry, s=s):
                g = pick(i, 15 - i)
                row_task(fields[s], fields[s + 1], 4 if s == 3 else 0, g)
                if s == 3:
                    out_copy(g).start()
                return carry

            lax.fori_loop(first + slope * s, last - s, task, 0)

    for step in range(8):
        if step + AHEAD < 8:
            send_columns(step + AHEAD)
        if step == 7:
            @pl.when(has_far)
            def _():
                for i in range(4):
                    far_copy(i).wait_recv()

            row_phase(1, 10, 1)
        own_copy(step).wait()
        for side, other in (("left", "right"), ("right", "left")):
            @pl.when(has[other])
            def _():
                col_copy(side, step).wait_recv()

        col_phase(step)
        if step < 4:
            @pl.when(direct)
            def _():
                far_copy(step).start()

            @pl.when(middle)
            def _():
                to_relay(step).start()
        else:
            near_copy(step).start()
        if 1 <= step < 5:
            @pl.when(is_relay)
            def _():
                to_relay(step - 1).wait_recv()
                from_relay(step - 1).start()

    for step in range(4, 8):
        near_copy(step).wait_recv()
    row_phase(10, 15, -1)

    for step in range(8):
        out_copy(4 + step).wait()
        for side in ("left", "right"):
            @pl.when(has[side])
            def _():
                col_copy(side, step).wait_send()

        if step < 4:
            @pl.when(has_far)
            def _():
                far_copy(step).wait_send()

            @pl.when(is_relay)
            def _():
                from_relay(step).wait_send()
        else:
            near_copy(step).wait_send()


def per_device(covariance, wind_x, wind_y, patch_map, kappa_table):
    f32 = jnp.float32
    dma = pltpu.SemaphoreType.DMA
    return pl.pallas_call(
        kernel,
        out_shape=jax.ShapeDtypeStruct(covariance.shape, f32),
        in_specs=[
            pl.BlockSpec(memory_space=pl.ANY),
            pl.BlockSpec(memory_space=pltpu.VMEM),
            pl.BlockSpec(memory_space=pltpu.VMEM),
            pl.BlockSpec(memory_space=pltpu.VMEM),
            pl.BlockSpec(memory_space=pltpu.SMEM),
        ],
        out_specs=pl.BlockSpec(memory_space=pl.ANY),
        scratch_shapes=[
            pltpu.VMEM((1024, 2048), f32),
            pltpu.VMEM((16, GY, 1024), f32),
            pltpu.VMEM((16, GY, 1024), f32),
            pltpu.VMEM((16, GY, 1024), f32),
            pltpu.VMEM((16, GY, 1024), f32),
            pltpu.VMEM((8, GY, 1024), f32),
            pltpu.VMEM((4, GY, 1024), f32),
            pltpu.VMEM((5, 14, 8, GY), f32),
            pltpu.VMEM((14, 5, GY, GY), f32),
            pltpu.VMEM((5, 144, GY), f32),
            dma((8,)),
            dma((8,)),
            dma((2, 8)),
            dma((2, 8)),
            dma((4,)),
            dma((4,)),
            dma((4,)),
            dma((4,)),
            dma((4,)),
            dma((4,)),
        ],
        compiler_params=pltpu.CompilerParams(
            collective_id=0, has_side_effects=True, vmem_limit_bytes=62 * 1024 * 1024
        ),
    )(covariance, wind_x, wind_y, patch_map, kappa_table)


def solution(mesh):
    return jax.shard_map(
        per_device,
        mesh=mesh,
        in_specs=(P("row", "col"), P(), P(), P(), P()),
        out_specs=P("row", "col"),
        check_vma=False,
    )
```

```python
import jax
import jax.numpy as jnp
from jax import lax
from jax.experimental import pallas as pl
from jax.experimental.pallas import tpu as pltpu
from jax.sharding import PartitionSpec as P

GY = 128
PATCHES = 16
MESH = pl.DeviceIdType.MESH
AHEAD = 2
HALF = 512


def coefficients(wind_x, wind_y, patch_map, kappa_table):
    kappa = jnp.zeros((GY, GY), jnp.float32)
    for label in range(PATCHES):
        kappa = jnp.where(patch_map[...] == label, kappa_table[label], kappa)
    y = lax.broadcasted_iota(jnp.int32, (GY, GY), 1)
    half_x, half_y = 0.5 * wind_x[...], 0.5 * wind_y[...]
    return (
        1.0 - 4.0 * kappa,
        kappa - half_x,
        kappa + half_x,
        jnp.where(y < GY - 1, kappa - half_y, 0.0),
        jnp.where(y > 0, kappa + half_y, 0.0),
    )


def kernel(
    cov, wind_x, wind_y, patch_map, kappa_table, out,
    wide, f0, f1, f2, f3, final, relay, lane_coef, sub_coef, padded,
    own_sem, out_sem, col_send, col_recv, far_send, far_recv, near_send, near_recv,
    relay_send, relay_recv,
):
    r, c = lax.axis_index("row"), lax.axis_index("col")
    rows, cols = lax.axis_size("row"), lax.axis_size("col")
    odd = lax.rem(r, 2)

    def pick(even_value, odd_value):
        return even_value + odd * (odd_value - even_value)

    near_row, far_row = pick(r + 1, r - 1), pick(r - 1, r + 1)
    has_far = jnp.logical_and(r > 0, r < rows - 1)
    middle = jnp.logical_or(r == 7, r == 8)
    grid_y, place = c // 4, lax.rem(c, 4)
    even = lax.rem(c, 2) == 0
    inner = jnp.logical_or(grid_y == 1, grid_y == 2)
    outer = jnp.logical_or(
        jnp.logical_and(grid_y == 0, even), jnp.logical_and(grid_y == 3, jnp.logical_not(even))
    )

    def straight(upward):
        return jnp.logical_or(outer, jnp.logical_and(inner, place // 2 == upward))

    opposite = jnp.where(inner, c, 4 * (3 - grid_y) + place)
    sends_straight, takes_straight = straight(r - 7), straight(8 - r)
    both, no = jnp.logical_and, jnp.logical_not
    half = r // 8
    outer_relay = both(no(has_far), jnp.logical_or(outer, both(inner, place // 2 != half)))
    inner_relay = both(inner, r == 2 + 8 * half + 2 * (place // 2))
    is_relay = jnp.logical_or(outer_relay, inner_relay)
    flow_from, flow_to = (7 + half, opposite), (8 - half, opposite)
    sent_to, taken_from = (15 * (r - 7), opposite), (15 * (8 - r), opposite)
    inner_sent_to = (2 + 8 * (r - 7) + 2 * (place // 2), c)
    inner_taken_from = (2 + 8 * (8 - r) + 2 * (place // 2), c)
    split = both(middle, inner)

    def direct(step):
        straight_here = both(sends_straight, no(inner)) if step < 2 else sends_straight
        return both(has_far, jnp.logical_or(no(middle), straight_here))

    def relayed(step):
        return both(middle, no(direct(step)))

    def relays(step):
        if step < 2:
            return jnp.logical_or(inner_relay, both(outer_relay, no(inner)))
        return outer_relay

    def relay_for(step):
        if step < 2:
            return tuple(jnp.where(inner, x, y) for x, y in zip(inner_sent_to, sent_to))
        return sent_to

    has = {"left": c > 0, "right": c < cols - 1}
    where = {"left": (r, c - 1), "right": (r, c + 1)}

    def chunk(step):
        return pick(step, 7 - step)

    def chunk_rows(step):
        return pl.ds(pl.multiple_of(chunk(step) * GY, GY), GY)

    def own_copy(step):
        return pltpu.make_async_copy(
            cov.at[chunk_rows(step), :], wide.at[chunk_rows(step), pl.ds(HALF, 1024)], own_sem.at[step]
        )

    for step in range(8):
        own_copy(step).start()

    barrier = pltpu.get_barrier_semaphore()
    peers = (
        (has["left"], where["left"]),
        (has["right"], where["right"]),
        (r >= 0, (near_row, c)),
        (both(has_far, jnp.logical_or(no(middle), sends_straight)), (far_row, c)),
        (both(middle, takes_straight), (far_row, c)),
        (both(middle, no(sends_straight)), sent_to),
        (both(middle, no(takes_straight)), taken_from),
        (split, inner_sent_to),
        (split, inner_taken_from),
        (is_relay, flow_from),
        (is_relay, flow_to),
    )
    for there, peer in peers:
        @pl.when(there)
        def _():
            pl.semaphore_signal(barrier, inc=1, device_id=peer, device_id_type=MESH)
    pl.semaphore_wait(barrier, sum(there.astype(jnp.int32) for there, _ in peers))

    def col_copy(side, step):
        i = 0 if side == "left" else 1
        return pltpu.make_async_remote_copy(
            src_ref=cov.at[chunk_rows(step), pl.ds(HALF * i, HALF)],
            dst_ref=wide.at[chunk_rows(step), pl.ds(1536 if i == 0 else 0, HALF)],
            send_sem=col_send.at[i, step],
            recv_sem=col_recv.at[i, step],
            device_id=where[side],
            device_id_type=MESH,
        )

    def send_columns(step):
        for side in ("left", "right"):
            @pl.when(has[side])
            def _():
                col_copy(side, step).start()

    def far_copy(step):
        return pltpu.make_async_remote_copy(
            src_ref=f0.at[4 + chunk(step)],
            dst_ref=f0.at[pick(12 + step, 3 - step)],
            send_sem=far_send.at[step],
            recv_sem=far_recv.at[step],
            device_id=(far_row, c),
            device_id_type=MESH,
        )

    def to_relay(step):
        return pltpu.make_async_remote_copy(
            src_ref=f0.at[4 + chunk(step)],
            dst_ref=relay.at[step],
            send_sem=far_send.at[step],
            recv_sem=relay_recv.at[step],
            device_id=relay_for(step),
            device_id_type=MESH,
        )

    def from_relay(step):
        return pltpu.make_async_remote_copy(
            src_ref=relay.at[step],
            dst_ref=f0.at[3 - step + half * (9 + 2 * step)],
            send_sem=relay_send.at[step],
            recv_sem=far_recv.at[step],
            device_id=flow_to,
            device_id_type=MESH,
        )

    def near_copy(step):
        return pltpu.make_async_remote_copy(
            src_ref=f0.at[4 + chunk(step)],
            dst_ref=f0.at[pick(step - 4, 19 - step)],
            send_sem=near_send.at[step - 4],
            recv_sem=near_recv.at[step - 4],
            device_id=(near_row, c),
            device_id_type=MESH,
        )

    for step in range(AHEAD):
        send_columns(step)

    maps = coefficients(wind_x, wind_y, patch_map, kappa_table)
    padded[...] = jnp.zeros_like(padded)
    for j in range(5):
        padded[j, pl.ds(8, GY), :] = maps[j]
    for j in range(5):
        window = padded[j, pl.ds(pl.multiple_of(8 * c, 8), 24), :]
        for w in range(14):
            lane_coef[j, w] = jnp.broadcast_to(window[5 + w : 6 + w, :], (8, GY))
    for j in range(5):
        turned = pltpu.roll(maps[j].T, lax.rem(132 - 8 * r, 128), 1)
        for w in range(14):
            place = 8 * r - 3 + w
            inside = jnp.logical_and(place >= 0, place < GY)
            column = jnp.broadcast_to(turned[:, w + 1 : w + 2], (GY, GY))
            sub_coef[w, j] = jnp.where(inside, column, 0.0)

    @pl.when(c == 0)
    def _():
        wide[:, pl.ds(0, HALF)] = jnp.zeros((1024, HALF), jnp.float32)

    @pl.when(c == cols - 1)
    def _():
        wide[:, pl.ds(1536, HALF)] = jnp.zeros((1024, HALF), jnp.float32)

    @pl.when(r == 0)
    def _():
        f0[pl.ds(0, 4)] = jnp.zeros((4, GY, 1024), jnp.float32)

    @pl.when(r == rows - 1)
    def _():
        f0[pl.ds(12, 4)] = jnp.zeros((4, GY, 1024), jnp.float32)

    def col_phase(step):
        k = chunk(step)

        def group(i, carry):
            base = pl.multiple_of(k * GY + i * 16, 16)
            inner = pl.multiple_of(i * 16, 16)
            slabs = [
                [wide[pl.ds(base + 8 * u, 8), pl.ds(GY * w, GY)] for u in range(2)] for w in range(16)
            ]
            for s in range(4):
                fresh = [None] * 16
                for w in range(s + 1, 15 - s):
                    cc, cn, cs, ce, cw = [lane_coef[j, w - 1] for j in range(5)]
                    fresh[w] = [
                        cc * slabs[w][u]
                        + cn * slabs[w + 1][u]
                        + cs * slabs[w - 1][u]
                        + ce * pltpu.roll(slabs[w][u], GY - 1, 1)
                        + cw * pltpu.roll(slabs[w][u], 1, 1)
                        for u in range(2)
                    ]
                slabs = fresh
            for w in range(4, 12):
                for u in range(2):
                    f0[4 + k, pl.ds(inner + 8 * u, 8), pl.ds(GY * (w - 4), GY)] = slabs[w][u]
            return carry

        lax.fori_loop(0, 8, group, 0)

    sub = lax.broadcasted_iota(jnp.int32, (8, GY), 0)

    def row_task(source, target, shift, g):
        def part(q, carry):
            lanes = [pl.ds(pl.multiple_of(q * 256 + GY * u, GY), GY) for u in range(2)]

            def load(grid, k, u):
                return source[grid, pl.ds(8 * k, 8), lanes[u]]

            here = [[load(g, 0, u) for u in range(2)]]
            ups = [[pltpu.roll(here[0][u], 7, 0) for u in range(2)]]
            last_down = [jnp.zeros((8, GY), jnp.float32)] * 2
            for k in range(16):
                if k < 15:
                    here.append([load(g, k + 1, u) for u in range(2)])
                    ups.append([pltpu.roll(here[k + 1][u], 7, 0) for u in range(2)])
                cc, cn, cs, ce, cw = [sub_coef[g - 1, j, pl.ds(8 * k, 8), :] for j in range(5)]
                for u in range(2):
                    down = pltpu.roll(here[k][u], 1, 0)
                    east = jnp.where(sub == 7, ups[k + 1][u], ups[k][u]) if k < 15 else ups[k][u]
                    west = jnp.where(sub == 0, last_down[u], down)
                    last_down[u] = down
                    target[g - shift, pl.ds(8 * k, 8), lanes[u]] = (
                        cc * here[k][u]
                        + cn * load(g + 1, k, u)
                        + cs * load(g - 1, k, u)
                        + ce * east
                        + cw * west
                    )
            return carry

        lax.fori_loop(0, 4, part, 0)

    def out_copy(g):
        return pltpu.make_async_copy(
            final.at[g - 4], out.at[pl.ds(pl.multiple_of((g - 4) * GY, GY), GY), :], out_sem.at[g - 4]
        )

    fields = (f0, f1, f2, f3, final)

    def row_phase(first, last, slope):
        for s in range(4):
            def task(i, carry, s=s):
                g = pick(i, 15 - i)
                row_task(fields[s], fields[s + 1], 4 if s == 3 else 0, g)
                if s == 3:
                    out_copy(g).start()
                return carry

            lax.fori_loop(first + slope * s, last - s, task, 0)

    for step in range(8):
        if step + AHEAD < 8:
            send_columns(step + AHEAD)
        if step == 7:
            @pl.when(has_far)
            def _():
                for i in range(4):
                    far_copy(i).wait_recv()

            row_phase(1, 10, 1)
        own_copy(step).wait()
        for side, other in (("left", "right"), ("right", "left")):
            @pl.when(has[other])
            def _():
                col_copy(side, step).wait_recv()

        col_phase(step)
        if step < 4:
            @pl.when(direct(step))
            def _():
                far_copy(step).start()

            @pl.when(relayed(step))
            def _():
                to_relay(step).start()
        else:
            near_copy(step).start()
        if 1 <= step < 5:
            @pl.when(relays(step - 1))
            def _():
                to_relay(step - 1).wait_recv()
                from_relay(step - 1).start()

    for step in range(4, 8):
        near_copy(step).wait_recv()
    row_phase(10, 15, -1)

    for step in range(8):
        out_copy(4 + step).wait()
        for side in ("left", "right"):
            @pl.when(has[side])
            def _():
                col_copy(side, step).wait_send()

        if step < 4:
            @pl.when(has_far)
            def _():
                far_copy(step).wait_send()

            @pl.when(relays(step))
            def _():
                from_relay(step).wait_send()
        else:
            near_copy(step).wait_send()


def per_device(covariance, wind_x, wind_y, patch_map, kappa_table):
    f32 = jnp.float32
    dma = pltpu.SemaphoreType.DMA
    return pl.pallas_call(
        kernel,
        out_shape=jax.ShapeDtypeStruct(covariance.shape, f32),
        in_specs=[
            pl.BlockSpec(memory_space=pl.ANY),
            pl.BlockSpec(memory_space=pltpu.VMEM),
            pl.BlockSpec(memory_space=pltpu.VMEM),
            pl.BlockSpec(memory_space=pltpu.VMEM),
            pl.BlockSpec(memory_space=pltpu.SMEM),
        ],
        out_specs=pl.BlockSpec(memory_space=pl.ANY),
        scratch_shapes=[
            pltpu.VMEM((1024, 2048), f32),
            pltpu.VMEM((16, GY, 1024), f32),
            pltpu.VMEM((16, GY, 1024), f32),
            pltpu.VMEM((16, GY, 1024), f32),
            pltpu.VMEM((16, GY, 1024), f32),
            pltpu.VMEM((8, GY, 1024), f32),
            pltpu.VMEM((4, GY, 1024), f32),
            pltpu.VMEM((5, 14, 8, GY), f32),
            pltpu.VMEM((14, 5, GY, GY), f32),
            pltpu.VMEM((5, 144, GY), f32),
            dma((8,)),
            dma((8,)),
            dma((2, 8)),
            dma((2, 8)),
            dma((4,)),
            dma((4,)),
            dma((4,)),
            dma((4,)),
            dma((4,)),
            dma((4,)),
        ],
        compiler_params=pltpu.CompilerParams(
            collective_id=0, has_side_effects=True, vmem_limit_bytes=62 * 1024 * 1024
        ),
    )(covariance, wind_x, wind_y, patch_map, kappa_table)


def solution(mesh):
    return jax.shard_map(
        per_device,
        mesh=mesh,
        in_specs=(P("row", "col"), P(), P(), P(), P()),
        out_specs=P("row", "col"),
        check_vma=False,
    )
```

```python
import jax
import jax.numpy as jnp
from jax import lax
from jax.experimental import pallas as pl
from jax.experimental.pallas import tpu as pltpu
from jax.sharding import PartitionSpec as P

GY = 128
PATCHES = 16
MESH = pl.DeviceIdType.MESH
AHEAD = 2
HALF = 512


def coefficients(wind_x, wind_y, patch_map, kappa_table):
    kappa = jnp.zeros((GY, GY), jnp.float32)
    for label in range(PATCHES):
        kappa = jnp.where(patch_map[...] == label, kappa_table[label], kappa)
    y = lax.broadcasted_iota(jnp.int32, (GY, GY), 1)
    half_x, half_y = 0.5 * wind_x[...], 0.5 * wind_y[...]
    return (
        1.0 - 4.0 * kappa,
        kappa - half_x,
        kappa + half_x,
        jnp.where(y < GY - 1, kappa - half_y, 0.0),
        jnp.where(y > 0, kappa + half_y, 0.0),
    )


def kernel(
    cov, wind_x, wind_y, patch_map, kappa_table, out,
    wide, f0, f1, f2, f3, final, relay, lane_coef, sub_coef, padded,
    own_sem, out_sem, col_send, col_recv, far_send, far_recv, near_send, near_recv,
    relay_send, relay_recv,
):
    r, c = lax.axis_index("row"), lax.axis_index("col")
    rows, cols = lax.axis_size("row"), lax.axis_size("col")
    odd = lax.rem(r, 2)

    def pick(even_value, odd_value):
        return even_value + odd * (odd_value - even_value)

    near_row, far_row = pick(r + 1, r - 1), pick(r - 1, r + 1)
    has_far = jnp.logical_and(r > 0, r < rows - 1)
    middle = jnp.logical_or(r == 7, r == 8)
    grid_y, place = c // 4, lax.rem(c, 4)
    even = lax.rem(c, 2) == 0
    inner = jnp.logical_or(grid_y == 1, grid_y == 2)
    outer = jnp.logical_or(
        jnp.logical_and(grid_y == 0, even), jnp.logical_and(grid_y == 3, jnp.logical_not(even))
    )

    def straight(upward):
        return jnp.logical_or(outer, jnp.logical_and(inner, place // 2 == upward))

    opposite = jnp.where(inner, c, 4 * (3 - grid_y) + place)
    sends_straight, takes_straight = straight(r - 7), straight(8 - r)
    both, no = jnp.logical_and, jnp.logical_not
    half = r // 8
    outer_relay = both(no(has_far), jnp.logical_or(outer, both(inner, place // 2 != half)))
    inner_relay = both(inner, r == 2 + 8 * half + 2 * (place // 2))
    is_relay = jnp.logical_or(outer_relay, inner_relay)
    flow_from, flow_to = (7 + half, opposite), (8 - half, opposite)
    sent_to, taken_from = (15 * (r - 7), opposite), (15 * (8 - r), opposite)
    inner_sent_to = (2 + 8 * (r - 7) + 2 * (place // 2), c)
    inner_taken_from = (2 + 8 * (8 - r) + 2 * (place // 2), c)
    split = both(middle, inner)

    def direct(step):
        straight_here = both(sends_straight, no(inner)) if step < 2 else sends_straight
        return both(has_far, jnp.logical_or(no(middle), straight_here))

    def relayed(step):
        return both(middle, no(direct(step)))

    def relays(step):
        if step < 2:
            return jnp.logical_or(inner_relay, both(outer_relay, no(inner)))
        return outer_relay

    def relay_for(step):
        if step < 2:
            return tuple(jnp.where(inner, x, y) for x, y in zip(inner_sent_to, sent_to))
        return sent_to

    has = {"left": c > 0, "right": c < cols - 1}
    where = {"left": (r, c - 1), "right": (r, c + 1)}

    def chunk(step):
        return pick(step, 7 - step)

    def chunk_rows(step):
        return pl.ds(pl.multiple_of(chunk(step) * GY, GY), GY)

    def own_copy(step):
        return pltpu.make_async_copy(
            cov.at[chunk_rows(step), :], wide.at[chunk_rows(step), pl.ds(HALF, 1024)], own_sem.at[step]
        )

    for step in range(8):
        own_copy(step).start()

    barrier = pltpu.get_barrier_semaphore()
    peers = (
        (has["left"], where["left"]),
        (has["right"], where["right"]),
        (r >= 0, (near_row, c)),
        (both(has_far, jnp.logical_or(no(middle), sends_straight)), (far_row, c)),
        (both(middle, takes_straight), (far_row, c)),
        (both(middle, no(sends_straight)), sent_to),
        (both(middle, no(takes_straight)), taken_from),
        (split, inner_sent_to),
        (split, inner_taken_from),
        (is_relay, flow_from),
        (is_relay, flow_to),
    )
    for there, peer in peers:
        @pl.when(there)
        def _():
            pl.semaphore_signal(barrier, inc=1, device_id=peer, device_id_type=MESH)
    pl.semaphore_wait(barrier, sum(there.astype(jnp.int32) for there, _ in peers))

    def col_copy(side, step):
        i = 0 if side == "left" else 1
        return pltpu.make_async_remote_copy(
            src_ref=cov.at[chunk_rows(step), pl.ds(HALF * i, HALF)],
            dst_ref=wide.at[chunk_rows(step), pl.ds(1536 if i == 0 else 0, HALF)],
            send_sem=col_send.at[i, step],
            recv_sem=col_recv.at[i, step],
            device_id=where[side],
            device_id_type=MESH,
        )

    def send_columns(step):
        for side in ("left", "right"):
            @pl.when(has[side])
            def _():
                col_copy(side, step).start()

    def far_copy(step):
        return pltpu.make_async_remote_copy(
            src_ref=f0.at[4 + chunk(step)],
            dst_ref=f0.at[pick(12 + step, 3 - step)],
            send_sem=far_send.at[step],
            recv_sem=far_recv.at[step],
            device_id=(far_row, c),
            device_id_type=MESH,
        )

    def to_relay(step):
        return pltpu.make_async_remote_copy(
            src_ref=f0.at[4 + chunk(step)],
            dst_ref=relay.at[step],
            send_sem=far_send.at[step],
            recv_sem=relay_recv.at[step],
            device_id=relay_for(step),
            device_id_type=MESH,
        )

    def from_relay(step):
        return pltpu.make_async_remote_copy(
            src_ref=relay.at[step],
            dst_ref=f0.at[3 - step + half * (9 + 2 * step)],
            send_sem=relay_send.at[step],
            recv_sem=far_recv.at[step],
            device_id=flow_to,
            device_id_type=MESH,
        )

    def near_copy(step):
        return pltpu.make_async_remote_copy(
            src_ref=f0.at[4 + chunk(step)],
            dst_ref=f0.at[pick(step - 4, 19 - step)],
            send_sem=near_send.at[step - 4],
            recv_sem=near_recv.at[step - 4],
            device_id=(near_row, c),
            device_id_type=MESH,
        )

    for step in range(AHEAD):
        send_columns(step)

    maps = coefficients(wind_x, wind_y, patch_map, kappa_table)
    padded[...] = jnp.zeros_like(padded)
    for j in range(5):
        padded[j, pl.ds(8, GY), :] = maps[j]
    for j in range(5):
        window = padded[j, pl.ds(pl.multiple_of(8 * c, 8), 24), :]
        for w in range(14):
            lane_coef[j, w] = jnp.broadcast_to(window[5 + w : 6 + w, :], (8, GY))
    for j in range(5):
        turned = pltpu.roll(maps[j].T, lax.rem(132 - 8 * r, 128), 1)
        for w in range(14):
            place = 8 * r - 3 + w
            inside = jnp.logical_and(place >= 0, place < GY)
            column = jnp.broadcast_to(turned[:, w + 1 : w + 2], (GY, GY))
            sub_coef[w, j] = jnp.where(inside, column, 0.0)

    @pl.when(c == 0)
    def _():
        wide[:, pl.ds(0, HALF)] = jnp.zeros((1024, HALF), jnp.float32)

    @pl.when(c == cols - 1)
    def _():
        wide[:, pl.ds(1536, HALF)] = jnp.zeros((1024, HALF), jnp.float32)

    @pl.when(r == 0)
    def _():
        f0[pl.ds(0, 4)] = jnp.zeros((4, GY, 1024), jnp.float32)

    @pl.when(r == rows - 1)
    def _():
        f0[pl.ds(12, 4)] = jnp.zeros((4, GY, 1024), jnp.float32)

    def col_phase(step):
        k = chunk(step)

        def group(i, carry):
            base = pl.multiple_of(k * GY + i * 16, 16)
            inner = pl.multiple_of(i * 16, 16)
            slabs = [
                [wide[pl.ds(base + 8 * u, 8), pl.ds(GY * w, GY)] for u in range(2)] for w in range(16)
            ]
            for s in range(4):
                fresh = [None] * 16
                for w in range(s + 1, 15 - s):
                    cc, cn, cs, ce, cw = [lane_coef[j, w - 1] for j in range(5)]
                    fresh[w] = [
                        cc * slabs[w][u]
                        + cn * slabs[w + 1][u]
                        + cs * slabs[w - 1][u]
                        + ce * pltpu.roll(slabs[w][u], GY - 1, 1)
                        + cw * pltpu.roll(slabs[w][u], 1, 1)
                        for u in range(2)
                    ]
                slabs = fresh
            for w in range(4, 12):
                for u in range(2):
                    f0[4 + k, pl.ds(inner + 8 * u, 8), pl.ds(GY * (w - 4), GY)] = slabs[w][u]
            return carry

        lax.fori_loop(0, 8, group, 0)

    sub = lax.broadcasted_iota(jnp.int32, (8, GY), 0)

    def row_task(source, target, shift, g):
        def part(q, carry):
            lanes = [pl.ds(pl.multiple_of(q * 256 + GY * u, GY), GY) for u in range(2)]

            def load(grid, k, u):
                return source[grid, pl.ds(8 * k, 8), lanes[u]]

            here = [[load(g, 0, u) for u in range(2)]]
            ups = [[pltpu.roll(here[0][u], 7, 0) for u in range(2)]]
            last_down = [jnp.zeros((8, GY), jnp.float32)] * 2
            for k in range(16):
                if k < 15:
                    here.append([load(g, k + 1, u) for u in range(2)])
                    ups.append([pltpu.roll(here[k + 1][u], 7, 0) for u in range(2)])
                cc, cn, cs, ce, cw = [sub_coef[g - 1, j, pl.ds(8 * k, 8), :] for j in range(5)]
                for u in range(2):
                    down = pltpu.roll(here[k][u], 1, 0)
                    east = jnp.where(sub == 7, ups[k + 1][u], ups[k][u]) if k < 15 else ups[k][u]
                    west = jnp.where(sub == 0, last_down[u], down)
                    last_down[u] = down
                    target[g - shift, pl.ds(8 * k, 8), lanes[u]] = (
                        cc * here[k][u]
                        + cn * load(g + 1, k, u)
                        + cs * load(g - 1, k, u)
                        + ce * east
                        + cw * west
                    )
            return carry

        lax.fori_loop(0, 4, part, 0)

    def out_copy(g):
        return pltpu.make_async_copy(
            final.at[g - 4], out.at[pl.ds(pl.multiple_of((g - 4) * GY, GY), GY), :], out_sem.at[g - 4]
        )

    fields = (f0, f1, f2, f3, final)

    def row_phase(first, last, slope):
        for s in range(4):
            def task(i, carry, s=s):
                g = pick(i, 15 - i)
                row_task(fields[s], fields[s + 1], 4 if s == 3 else 0, g)
                if s == 3:
                    out_copy(g).start()
                return carry

            lax.fori_loop(first + slope * s, last - s, task, 0)

    for step in range(8):
        if step + AHEAD < 8:
            send_columns(step + AHEAD)
        if step == 7:
            @pl.when(has_far)
            def _():
                for i in range(4):
                    far_copy(i).wait_recv()

            row_phase(1, 10, 1)
        own_copy(step).wait()
        for side, other in (("left", "right"), ("right", "left")):
            @pl.when(has[other])
            def _():
                col_copy(side, step).wait_recv()

        col_phase(step)
        if step < 4:
            @pl.when(direct(step))
            def _():
                far_copy(step).start()

            @pl.when(relayed(step))
            def _():
                to_relay(step).start()
        else:
            near_copy(step).start()
        if 1 <= step < 5:
            @pl.when(relays(step - 1))
            def _():
                to_relay(step - 1).wait_recv()
                from_relay(step - 1).start()

    for step in range(4, 8):
        near_copy(step).wait_recv()
    row_phase(10, 15, -1)

    for step in range(8):
        out_copy(4 + step).wait()
        for side in ("left", "right"):
            @pl.when(has[side])
            def _():
                col_copy(side, step).wait_send()

        if step < 4:
            @pl.when(has_far)
            def _():
                far_copy(step).wait_send()

            @pl.when(relays(step))
            def _():
                from_relay(step).wait_send()
        else:
            near_copy(step).wait_send()


def hand_over(source, target, stage, read_sem, write_sem):
    parts = [pl.ds(k * GY, GY) for k in range(8)]
    reads = [pltpu.make_async_copy(source.at[p], stage.at[p], read_sem.at[k]) for k, p in enumerate(parts)]
    writes = [pltpu.make_async_copy(stage.at[p], target.at[p], write_sem.at[k]) for k, p in enumerate(parts)]
    for read in reads:
        read.start()
    for read, write in zip(reads, writes):
        read.wait()
        write.start()
    for write in writes:
        write.wait()


def per_device(covariance, wind_x, wind_y, patch_map, kappa_table):
    f32 = jnp.float32
    dma = pltpu.SemaphoreType.DMA
    forecast = pl.pallas_call(
        kernel,
        out_shape=jax.ShapeDtypeStruct(covariance.shape, f32),
        in_specs=[
            pl.BlockSpec(memory_space=pl.ANY),
            pl.BlockSpec(memory_space=pltpu.VMEM),
            pl.BlockSpec(memory_space=pltpu.VMEM),
            pl.BlockSpec(memory_space=pltpu.VMEM),
            pl.BlockSpec(memory_space=pltpu.SMEM),
        ],
        out_specs=pl.BlockSpec(memory_space=pl.ANY),
        scratch_shapes=[
            pltpu.VMEM((1024, 2048), f32),
            pltpu.VMEM((16, GY, 1024), f32),
            pltpu.VMEM((16, GY, 1024), f32),
            pltpu.VMEM((16, GY, 1024), f32),
            pltpu.VMEM((16, GY, 1024), f32),
            pltpu.VMEM((8, GY, 1024), f32),
            pltpu.VMEM((4, GY, 1024), f32),
            pltpu.VMEM((5, 14, 8, GY), f32),
            pltpu.VMEM((14, 5, GY, GY), f32),
            pltpu.VMEM((5, 144, GY), f32),
            dma((8,)),
            dma((8,)),
            dma((2, 8)),
            dma((2, 8)),
            dma((4,)),
            dma((4,)),
            dma((4,)),
            dma((4,)),
            dma((4,)),
            dma((4,)),
        ],
        compiler_params=pltpu.CompilerParams(
            collective_id=0, has_side_effects=True, vmem_limit_bytes=62 * 1024 * 1024
        ),
    )(covariance, wind_x, wind_y, patch_map, kappa_table)
    return pl.pallas_call(
        hand_over,
        out_shape=jax.ShapeDtypeStruct(covariance.shape, f32),
        in_specs=[pl.BlockSpec(memory_space=pl.ANY)],
        out_specs=pl.BlockSpec(memory_space=pl.ANY),
        scratch_shapes=[pltpu.VMEM((1024, 1024), f32), dma((8,)), dma((8,))],
    )(forecast)


def solution(mesh):
    return jax.shard_map(
        per_device,
        mesh=mesh,
        in_specs=(P("row", "col"), P(), P(), P(), P()),
        out_specs=P("row", "col"),
        check_vma=False,
    )
```
